32 devices in a mesh: pipe: 2 (over x), tensor: 4 (over y, core), expert: 4 (over z).
Axes of the slice: x: 2, y: 2, z: 4, core: 2. Of those that a mesh axis runs over, the one named last changes fastest.
Arguments:
- tokens: bfloat16 [2, 256, 4096], P(None, 'expert'), may hold values from -6 to 6
- gains: float32 [2, 4096], P('pipe'), may hold values from 0.1 to 1.9
- route_ids: int32 [2, 2, 256, 2], P('pipe', None, 'expert'), may hold values from 0 to 3, all different within a row
- route_weights: float32 [2, 2, 256, 2], P('pipe', None, 'expert'), may hold values from 0.2 to 1
- picks: int32 [2, 2, 4, 64], P('pipe', None, 'expert'), may hold values from 0 to 63, each once within a row
- w_gate: bfloat16 [2, 4, 4096, 1536], P('pipe', 'expert', None, 'tensor'), may hold values from -0.09375 to 0.09375
- w_up: bfloat16 [2, 4, 4096, 1536], P('pipe', 'expert', None, 'tensor'), may hold values from -0.09375 to 0.09375
- w_down: bfloat16 [2, 4, 1536, 4096], P('pipe', 'expert', 'tensor'), may hold values from -0.15625 to 0.15625
Outputs:
- streams: bfloat16 [2, 2, 256, 4096], P('pipe', None, 'expert', 'tensor')
The draws below stay inside these ranges and needn't reach their ends.
Inputs may be any that keep to these rules, and one draw needn't show every extreme that they name: `route_ids`: each token names 2 different experts; every expert is named by some token. `picks`: for every layer, micro-batch and block of 64 tokens, a permutation of 0 to 63.
All inputs are finite; a program needn't handle non-finite values.
Results may differ from the reference program's by a relative error of at most 0.025.
Values may be sent and summed in bfloat16 or wider, within the bound.
A program may use at most 64 MiB of HBM per device.

```python
import jax
import jax.numpy as jnp
from jax import lax

D = 4096
FF = 1536
TOPK = 2
MICRO = 2
TOK_DEV = 64
EXPERTS = 4
QUARTER = 16
CAP = 10
TOKENS = 256
N_PIPE = 2
N_TENSOR = 4
N_EXPERT = 4


def steps_of(rng, shape, shards, low, top_value):
    loudness, own = 1.0, jax.random.fold_in(rng, 6)
    for dim, parts in shards:
        steps = jnp.exp(jax.random.uniform(jax.random.fold_in(own, dim), (parts,), jnp.float32, low / len(shards), top_value / len(shards)))
        loudness = loudness * jnp.repeat(steps, shape[dim] // parts).reshape([-1 if axis == dim else 1 for axis in range(len(shape))])
    return loudness


def different_ones(stream_key, rows, number_of, top, lift):
    sequence = jax.random.permutation(jax.random.fold_in(stream_key, 1), number_of)
    pull = sequence
    for power in range(3):
        pull = pull * pull // number_of
    pull = pull * lift // number_of
    lots = jax.random.randint(jax.random.fold_in(stream_key, 2), (rows, number_of), 0, 4096) + pull
    fixed_rows = jax.random.permutation(jax.random.fold_in(stream_key, 3), rows)[jnp.arange(number_of) % rows]
    lots = jnp.where(jnp.arange(rows)[:, None] == fixed_rows[None, :], 1 << 14, lots)
    priority = lots * number_of + jnp.arange(number_of)
    return lax.top_k(priority.astype(jnp.int32), top)[1].astype(jnp.int32)


def gaussian(key, shape, deviation, most, pieces=(), kind=jnp.bfloat16):
    values = jax.random.normal(key, shape, jnp.float32) * deviation
    if len(pieces) > 0:
        values = steps_of(key, shape, pieces, -0.22, 0.18) * values
    return jnp.clip(values, min=-most, max=most).astype(kind)


def setup_inputs(seed: int = 0) -> dict:
    key_list = jax.random.split(jax.random.key(seed), 9)
    tokens = gaussian(key_list[0], (MICRO, TOKENS, D), 1.0, 6.0, ((1, 4),))
    gains = jnp.clip(1.0 + 0.18 * jax.random.normal(key_list[1], (N_PIPE, D), jnp.float32), 0.1, 1.9)
    route_ids = different_ones(key_list[2], N_PIPE * MICRO * TOKENS, EXPERTS, TOPK, 8192).reshape((N_PIPE, MICRO, TOKENS, TOPK))
    route_weights = jnp.clip(0.2 + 0.8 * jax.random.uniform(key_list[3], (N_PIPE, MICRO, TOKENS, TOPK), jnp.float32) ** steps_of(key_list[3], (N_PIPE, MICRO, TOKENS, TOPK), ((0, 2), (2, 4)), -0.2, 0.2), 0.2, 1.0)
    picks = jax.vmap(lambda own: jax.random.permutation(own, TOK_DEV))(jax.random.split(key_list[4], N_PIPE * MICRO * N_EXPERT)).reshape((N_PIPE, MICRO, N_EXPERT, TOK_DEV)).astype(jnp.int32)
    w_gate = gaussian(key_list[5], (N_PIPE, EXPERTS, D, FF), D ** -0.5, 0.09375, ((0, 2), (1, 4), (3, 4)))
    w_up = gaussian(key_list[6], (N_PIPE, EXPERTS, D, FF), D ** -0.5, 0.09375, ((0, 2), (1, 4), (3, 4)))
    w_down = gaussian(key_list[7], (N_PIPE, EXPERTS, FF, D), FF ** -0.5, 0.15625, ((0, 2), (1, 4), (2, 4)))
    return dict(tokens=tokens, gains=gains, route_ids=route_ids, route_weights=route_weights, picks=picks, w_gate=w_gate, w_up=w_up, w_down=w_down)


epsilon = 1e-06

def find_slots(ordered_ids, capacity):
    onehot = (ordered_ids[..., None] == jnp.arange(EXPERTS, dtype=jnp.int32)).astype(jnp.int32)
    earlier = jnp.cumsum(onehot, axis=-2) - onehot
    slot_index = lax.optimization_barrier(jnp.sum(earlier * onehot, axis=-1))
    return (slot_index, slot_index < capacity)

def expert_ffn(operands):
    row_block, gate_matrix, up_matrix, down_matrix = operands
    gate_val = jnp.dot(row_block, gate_matrix, preferred_element_type=jnp.float32)
    up_val = jnp.dot(row_block, up_matrix, preferred_element_type=jnp.float32)
    hidden = (jax.nn.silu(gate_val) * up_val).astype(jnp.bfloat16)
    shard_width = FF // N_TENSOR
    summed = jnp.zeros((row_block.shape[0], D), jnp.float32)
    for shard_index in range(N_TENSOR):
        lower = shard_index * shard_width
        partial_sum = jnp.dot(hidden[:, lower:lower + shard_width], down_matrix[lower:lower + shard_width], preferred_element_type=jnp.float32)
        rounded = lax.optimization_barrier(partial_sum.astype(jnp.bfloat16))
        summed = summed + rounded.astype(jnp.float32)
    return summed.astype(jnp.bfloat16)

def moe_section(stream, gain_row, section_ids, section_weights, section_picks, gate_all, up_all, down_all):
    groups = N_EXPERT
    offsets = (jnp.arange(groups, dtype=jnp.int32) * TOK_DEV)[:, None]
    ordered = (section_picks + offsets).astype(jnp.int32).reshape(groups, N_TENSOR, QUARTER)
    stream_f = stream.astype(jnp.float32)
    inv_rms = lax.rsqrt(lax.optimization_barrier(jnp.mean(stream_f * stream_f, axis=1, keepdims=True)) + epsilon)
    normed = (stream_f * inv_rms * gain_row[None, :]).astype(jnp.bfloat16)
    ordered_ids = section_ids[ordered].reshape(groups, N_TENSOR, QUARTER * TOPK)
    ordered_weights = section_weights[ordered].reshape(groups, N_TENSOR, QUARTER * TOPK)
    slot_index, kept_mask = find_slots(ordered_ids, CAP)
    route_tokens = jnp.repeat(ordered, TOPK, axis=2)
    group_index = jnp.arange(groups, dtype=jnp.int32)[:, None, None]
    rank_index = jnp.arange(N_TENSOR, dtype=jnp.int32)[None, :, None]
    position = ((ordered_ids * groups + group_index) * N_TENSOR + rank_index) * CAP + slot_index
    filled = EXPERTS * groups * N_TENSOR * CAP
    target = jnp.where(kept_mask, position, filled).astype(jnp.int32)
    source = jnp.full((filled + 1,), TOKENS, jnp.int32).at[target.reshape(-1)].set(route_tokens.reshape(-1))
    padded = jnp.concatenate([normed, jnp.zeros((1, D), jnp.bfloat16)], axis=0)
    row_block = padded[source[:filled]].reshape(EXPERTS, groups * N_TENSOR * CAP, D)
    results = lax.map(expert_ffn, (row_block, gate_all, up_all, down_all))
    flat_results = jnp.concatenate([results.reshape(filled, D), jnp.zeros((1, D), jnp.bfloat16)], axis=0)
    picked = flat_results[target].astype(jnp.float32)
    weighted = picked * (ordered_weights * kept_mask)[..., None]
    update = lax.optimization_barrier(jnp.sum(weighted.reshape(groups, N_TENSOR, QUARTER, TOPK, D), axis=3))
    stream_new = stream_f.at[ordered.reshape(-1)].add(update.reshape(-1, D))
    return stream_new.astype(jnp.bfloat16)

def reference(tokens, gains, route_ids, route_weights, picks, w_gate, w_up, w_down):
    finished = []
    for micro_index in range(MICRO):
        stream = tokens[micro_index]
        column = []
        for section_index in range(N_PIPE):
            stream = moe_section(stream, gains[section_index], route_ids[section_index, micro_index], route_weights[section_index, micro_index], picks[section_index, micro_index], w_gate[section_index], w_up[section_index], w_down[section_index])
            column.append(stream)
        finished.append(jnp.stack(column))
    return jnp.stack(finished, axis=1)
```

```python
import functools

import jax
import jax.numpy as jnp
from jax import lax
from jax.experimental import pallas as pl
from jax.experimental.pallas import tpu as pltpu
from jax.sharding import PartitionSpec as P

epsilon = 1e-06
MESH = pl.DeviceIdType.MESH
F32 = jnp.float32
BF16 = jnp.bfloat16


def layer_kernel(
    sizes, tokens, gains, placing, comb, w_gate, w_up, w_down, out,
    h_in, fresh, send, x, wg, wu, wd, g_acc, u_acc, own, p_send, p_recv,
    y_send, y_recv, z_send, ret,
    w_sem, h_loc, h_send, h_recv, d_send, d_recv, f_send, f_recv, c_send, c_recv,
    ps_sem, pr_sem, ys_sem, yr_sem, zs_sem, zr_sem,
):
    micros, n_p, n_t, n_e, pair, rows_ge, width = sizes
    n_a = n_t // pair
    cut = (n_e + 1) // 2
    halves = [list(range(cut)), list(range(cut, n_e))]
    p = lax.axis_index("pipe")
    r = lax.axis_index("tensor")
    z = lax.axis_index("expert")
    a = lax.div(r, pair)
    c = lax.rem(r, pair)

    def peer_e(d):
        return lax.rem(z + d, n_e)

    def rank_of(da, dc):
        return lax.rem(a + da, n_a) * pair + lax.rem(c + dc, pair)

    def remote(src, dst, ssem, rsem, where):
        return pltpu.make_async_remote_copy(
            src_ref=src, dst_ref=dst, send_sem=ssem, recv_sem=rsem,
            device_id=where, device_id_type=MESH,
        )

    loads = [
        pltpu.make_async_copy(w_gate.at[0, 0], wg, w_sem.at[0]),
        pltpu.make_async_copy(w_up.at[0, 0], wu, w_sem.at[1]),
        pltpu.make_async_copy(w_down.at[0, 0], wd, w_sem.at[2]),
    ]

    def first_load(m):
        cols = pl.ds(pl.multiple_of(r * width, width), width)
        return pltpu.make_async_copy(tokens.at[m, :, cols], h_in.at[m], h_loc.at[m])

    @pl.when(p == 0)
    def _():
        for m in range(micros):
            first_load(m).start()

    for load in loads:
        load.start()

    barrier = pltpu.get_barrier_semaphore()

    def greet(where):
        pl.semaphore_signal(barrier, inc=1, device_id=where, device_id_type=MESH)

    for d in range(1, n_e):
        greet({"expert": peer_e(d)})
    for da in range(1, n_a):
        greet({"tensor": rank_of(da, 0)})
    for dc in range(1, pair):
        greet({"tensor": rank_of(0, dc)})

    @pl.when(p > 0)
    def _():
        greet({"pipe": p - 1})

    @pl.when(p < n_p - 1)
    def _():
        greet({"pipe": p + 1})

    ends = jnp.where(p > 0, 1, 0) + jnp.where(p < n_p - 1, 1, 0)
    pl.semaphore_wait(barrier, n_e - 1 + n_a - 1 + pair - 1 + ends)

    def relay(m):
        return remote(fresh.at[m], h_in.at[m], h_send.at[m], h_recv.at[m],
                      {"pipe": jnp.minimum(p + 1, n_p - 1)})

    def d_copy(m, d):
        return remote(send.at[m, d], x.at[m, r, z], d_send.at[m, d], d_recv.at[m, d],
                      {"expert": peer_e(d)})

    def f_copy(m, d, da):
        block = x.at[m, r, peer_e(n_e - d)]
        return remote(block, block, f_send.at[m, d, da], f_recv.at[m, d, da],
                      {"tensor": rank_of(da, 0)})

    def c_copy(m, d, da):
        block = x.at[m, rank_of(da, 0), peer_e(n_e - d)]
        return remote(block, block, c_send.at[m, d, da], c_recv.at[m, d, da],
                      {"tensor": rank_of(0, 1)})

    def p_copy(m, h, da):
        return remote(p_send.at[m, h, da], p_recv.at[m, h, da], ps_sem.at[m, h, da],
                      pr_sem.at[m, h, da], {"tensor": rank_of(0, 1)})

    def y_copy(m, d, da):
        return remote(y_send.at[m, d, da], y_recv.at[m, d, da], ys_sem.at[m, d, da],
                      yr_sem.at[m, d, da], {"tensor": rank_of(da, 0)})

    def z_copy(m, d):
        return remote(z_send.at[m, d], ret.at[m, z], zs_sem.at[m, d], zr_sem.at[m, d],
                      {"expert": peer_e(n_e - d)})

    def dispatch(m):
        @pl.when(p == 0)
        def _():
            first_load(m).wait()

        @pl.when(p > 0)
        def _():
            relay(m).wait_recv()

        h = h_in[m]
        for d in list(range(1, n_e)) + [0]:
            block = jnp.dot(placing[m, peer_e(d)], h, preferred_element_type=F32).astype(BF16)
            if d:
                send[m, d] = block
                d_copy(m, d).start()
            else:
                x[m, r, z] = block

    def forward(m, d):
        if d:
            d_copy(m, d).wait_recv()
        for da in range(1, n_a):
            f_copy(m, d, da).start()
        if pair > 1:
            c_copy(m, d, 0).start()

    def pass_on(m, d):
        for da in range(1, n_a):
            f_copy(m, d, da).wait_recv()
            if pair > 1:
                c_copy(m, d, da).start()

    def compute(m, h):
        if m == 0 and h == 0:
            for load in loads:
                load.wait()
        if pair > 1:
            for d in halves[h]:
                for da in range(n_a):
                    c_copy(m, d, da).wait_recv()
        homes = [peer_e(n_e - d) for d in halves[h]]

        def rows_of(q):
            return jnp.concatenate([x[m, q, g].astype(F32) for g in homes], axis=0)

        ss = jnp.zeros((len(homes) * rows_ge, 1), F32)
        for q in range(n_t):
            xf = rows_of(q)
            ss = ss + jnp.sum(xf * xf, axis=-1, keepdims=True)
        inv = lax.rsqrt(ss * (1.0 / (n_t * width)) + epsilon)
        for q in range(n_t):
            cols = slice(q * width, (q + 1) * width)
            nq = (rows_of(q) * inv * gains[0:1, cols]).astype(BF16)
            gq = jnp.dot(nq, wg[cols, :], preferred_element_type=F32)
            uq = jnp.dot(nq, wu[cols, :], preferred_element_type=F32)
            if q == 0:
                g_acc[...] = gq
                u_acc[...] = uq
            else:
                g_acc[...] += gq
                u_acc[...] += uq
        gate = g_acc[...]
        hidden = (gate / (1.0 + jnp.exp(-gate)) * u_acc[...]).astype(BF16)
        for dc in list(range(1, pair)) + [0]:
            for da in list(range(1, n_a)) + [0]:
                start = pl.multiple_of(rank_of(da, dc) * width, width)
                part = jnp.dot(hidden, wd[:, pl.ds(start, width)], preferred_element_type=F32)
                if dc:
                    p_send[m, h, da] = part.astype(BF16)
                    p_copy(m, h, da).start()
                else:
                    own[m, h, da] = part.astype(BF16)

    def reduce_pair(m, h):
        for da in list(range(1, n_a)) + [0]:
            if pair > 1:
                p_copy(m, h, da).wait_recv()
            for i, d in enumerate(halves[h]):
                part = slice(i * rows_ge, (i + 1) * rows_ge)
                total = own[m, h, da, part].astype(F32)
                if pair > 1:
                    total = total + p_recv[m, h, da, part].astype(F32)
                y_send[m, d, da] = total.astype(BF16)
                if da:
                    y_copy(m, d, da).start()

    def reduce_far(m, d):
        total = y_send[m, d, 0].astype(F32)
        for da in range(1, n_a):
            y_copy(m, d, da).wait_recv()
            total = total + y_recv[m, d, da].astype(F32)
        if d:
            z_send[m, d] = total.astype(BF16)
            z_copy(m, d).start()
        else:
            ret[m, z] = total.astype(BF16)

    def combine(m):
        toks = h_in.shape[1]
        for d in range(n_e):
            e = peer_e(d)
            if d:
                z_copy(m, d).wait_recv()
            both = jnp.dot(comb[m, e], ret[m, e], preferred_element_type=F32)
            g_part = both[:toks] + both[toks:]
            update = g_part if d == 0 else update + g_part
        new = (h_in[m].astype(F32) + update).astype(BF16)
        fresh[m] = new
        out[0, m] = new

        @pl.when(p < n_p - 1)
        def _():
            relay(m).start()

    near, far = halves[0], halves[-1]

    def step(fn, *args):
        return functools.partial(fn, *args)

    def head(m):
        steps = [step(forward, m, d) for d in near]
        steps += [step(pass_on, m, d) for d in near[:-1]]
        steps += [step(forward, m, far[0]), step(pass_on, m, near[-1])]
        return steps

    def middle(m):
        steps = [step(compute, m, 0)]
        steps += [step(forward, m, d) for d in far[1:]]
        steps += [step(pass_on, m, d) for d in far[:-1]]
        steps += [step(reduce_pair, m, 0), step(pass_on, m, far[-1])]
        return steps

    def back(m):
        return [step(compute, m, 1), step(reduce_pair, m, 1)]

    def tail(m):
        return [step(reduce_far, m, d) for d in near[1:] + near[:1] + far]

    def both_of(one, two):
        mixed = []
        for i in range(max(len(one), len(two))):
            mixed += one[i:i + 1] + two[i:i + 1]
        return mixed

    dispatch(0)

    @pl.when(p == 0)
    def _():
        for m in range(1, micros):
            dispatch(m)

    def late_dispatch(m):
        @pl.when(p > 0)
        def _():
            dispatch(m)

    plan = head(0)
    for m in range(micros):
        plan += middle(m)
        if m:
            plan += [step(combine, m - 1)]
        plan += back(m)
        if m + 1 < micros:
            plan += [step(late_dispatch, m + 1)]
            plan += both_of(tail(m), head(m + 1))
    plan += tail(micros - 1) + [step(combine, micros - 1)]
    for go in plan:
        go()

    for m in range(micros):
        for d in range(n_e):
            if d:
                d_copy(m, d).wait_send()
                z_copy(m, d).wait_send()
            for da in range(n_a):
                if da:
                    f_copy(m, d, da).wait_send()
                    y_copy(m, d, da).wait_send()
                if pair > 1:
                    c_copy(m, d, da).wait_send()
        if pair > 1:
            for h in range(len(halves)):
                for da in range(n_a):
                    p_copy(m, h, da).wait_send()

        @pl.when(p < n_p - 1)
        def _():
            relay(m).wait_send()


def local(mesh_shape, tokens, gains, route_ids, route_weights, picks, w_gate, w_up, w_down):
    n_p, n_t, n_e = mesh_shape
    micros, toks, model_width = tokens.shape
    route_count = route_ids.shape[3]
    quarter = toks // n_t
    capacity = 4 * quarter * route_count // (3 * n_e)
    width = model_width // n_t
    pair = 2 if n_t % 2 == 0 else 1
    n_a = n_t // pair
    rows_ge = -(-n_t * capacity // 8) * 8
    cut = (n_e + 1) // 2
    rows = cut * rows_ge
    hidden_width = w_gate.shape[3]

    ids = route_ids[0]
    weights = route_weights[0]
    order = picks[0, :, 0]
    each = jnp.arange(toks, dtype=jnp.int32)
    experts = jnp.arange(n_e, dtype=jnp.int32)
    hit = order[:, None, :] == each[None, :, None]
    pos = jnp.sum(jnp.where(hit, each[None, None, :], 0), axis=2)
    block = pos // quarter
    named = ids[:, :, :, None] == experts
    names = jnp.any(named, axis=2)
    w_te = jnp.sum(jnp.where(named, weights[..., None], 0.0), axis=2)
    before = (block[:, :, None] == block[:, None, :]) & (pos[:, None, :] < pos[:, :, None])
    slot = jnp.sum((before[..., None] & names[:, None]).astype(jnp.int32), axis=2)
    target = jnp.where(names & (slot < capacity), block[..., None] * capacity + slot, -1)
    target = target.transpose(0, 2, 1)
    w_et = w_te.transpose(0, 2, 1)
    places = jnp.arange(rows_ge, dtype=jnp.int32)
    placing = (places[None, None, :, None] == target[:, :, None, :]).astype(BF16)
    spread = target[..., None] == places
    high = lax.reduce_precision(w_et, 8, 7)
    low = w_et - high
    comb = jnp.concatenate(
        [jnp.where(spread, high[..., None], 0.0), jnp.where(spread, low[..., None], 0.0)], axis=2
    ).astype(BF16)

    sizes = (micros, n_p, n_t, n_e, pair, rows_ge, width)
    dma = pltpu.SemaphoreType.DMA
    vmem = pl.BlockSpec(memory_space=pltpu.VMEM)
    anywhere = pl.BlockSpec(memory_space=pl.ANY)
    return pl.pallas_call(
        functools.partial(layer_kernel, sizes),
        out_shape=jax.ShapeDtypeStruct((1, micros, toks, width), BF16),
        in_specs=[anywhere, vmem, vmem, vmem, anywhere, anywhere, anywhere],
        out_specs=vmem,
        scratch_shapes=[
            pltpu.VMEM((micros, toks, width), BF16),
            pltpu.VMEM((micros, toks, width), BF16),
            pltpu.VMEM((micros, n_e, rows_ge, width), BF16),
            pltpu.VMEM((micros, n_t, n_e, rows_ge, width), BF16),
            pltpu.VMEM(w_gate.shape[2:], BF16),
            pltpu.VMEM(w_up.shape[2:], BF16),
            pltpu.VMEM(w_down.shape[2:], BF16),
            pltpu.VMEM((rows, hidden_width), F32),
            pltpu.VMEM((rows, hidden_width), F32),
            pltpu.VMEM((micros, 2, n_a, rows, width), BF16),
            pltpu.VMEM((micros, 2, n_a, rows, width), BF16),
            pltpu.VMEM((micros, 2, n_a, rows, width), BF16),
            pltpu.VMEM((micros, n_e, n_a, rows_ge, width), BF16),
            pltpu.VMEM((micros, n_e, n_a, rows_ge, width), BF16),
            pltpu.VMEM((micros, n_e, rows_ge, width), BF16),
            pltpu.VMEM((micros, n_e, rows_ge, width), BF16),
            dma((3,)), dma((micros,)), dma((micros,)), dma((micros,)),
            dma((micros, n_e)), dma((micros, n_e)),
            dma((micros, n_e, n_a)), dma((micros, n_e, n_a)),
            dma((micros, n_e, n_a)), dma((micros, n_e, n_a)),
            dma((micros, 2, n_a)), dma((micros, 2, n_a)),
            dma((micros, n_e, n_a)), dma((micros, n_e, n_a)),
            dma((micros, n_e)), dma((micros, n_e)),
        ],
        compiler_params=pltpu.CompilerParams(
            collective_id=0, has_side_effects=True, vmem_limit_bytes=67043328
        ),
    )(tokens, gains, placing, comb, w_gate, w_up, w_down)


def solution(mesh):
    mesh_shape = (mesh.shape["pipe"], mesh.shape["tensor"], mesh.shape["expert"])
    return jax.shard_map(
        functools.partial(local, mesh_shape),
        mesh=mesh,
        in_specs=(
            P(None, "expert", None),
            P("pipe", None),
            P("pipe", None, "expert", None),
            P("pipe", None, "expert", None),
            P("pipe", None, "expert", None),
            P("pipe", "expert", None, "tensor"),
            P("pipe", "expert", None, "tensor"),
            P("pipe", "expert", "tensor", None),
        ),
        out_specs=P("pipe", None, "expert", "tensor"),
        check_vma=False,
    )
```

```python
import functools

import jax
import jax.numpy as jnp
from jax import lax
from jax.experimental import pallas as pl
from jax.experimental.pallas import tpu as pltpu
from jax.sharding import PartitionSpec as P

epsilon = 1e-06
MESH = pl.DeviceIdType.MESH
F32 = jnp.float32
BF16 = jnp.bfloat16


def layer_kernel(
    sizes, tokens, gains, ids, weights, picks, w_gate, w_up, w_down, out,
    placing, comb, h_in, fresh, send, x, wg, wu, wd, g_acc, u_acc, own, p_send, p_recv,
    y_send, y_recv, z_send, ret,
    w_sem, h_loc, h_send, h_recv, d_send, d_recv, f_send, f_recv, c_send, c_recv,
    ps_sem, pr_sem, ys_sem, yr_sem, zs_sem, zr_sem,
):
    micros, n_p, n_t, n_e, pair, rows_ge, width, capacity = sizes
    n_a = n_t // pair
    cut = (n_e + 1) // 2
    halves = [list(range(n_e - 1, cut - 1, -1)), list(range(cut - 1, -1, -1))]
    p = lax.axis_index("pipe")
    r = lax.axis_index("tensor")
    z = lax.axis_index("expert")
    a = lax.div(r, pair)
    c = lax.rem(r, pair)

    def peer_e(d):
        return lax.rem(z + d, n_e)

    def rank_of(da, dc):
        return lax.rem(a + da, n_a) * pair + lax.rem(c + dc, pair)

    def remote(src, dst, ssem, rsem, where):
        return pltpu.make_async_remote_copy(
            src_ref=src, dst_ref=dst, send_sem=ssem, recv_sem=rsem,
            device_id=where, device_id_type=MESH,
        )

    loads = [
        pltpu.make_async_copy(w_gate.at[0, 0], wg, w_sem.at[0]),
        pltpu.make_async_copy(w_up.at[0, 0], wu, w_sem.at[1]),
        pltpu.make_async_copy(w_down.at[0, 0], wd, w_sem.at[2]),
    ]

    def first_load(m):
        cols = pl.ds(pl.multiple_of(r * width, width), width)
        return pltpu.make_async_copy(tokens.at[m, :, cols], h_in.at[m], h_loc.at[m])

    @pl.when(p == 0)
    def _():
        for m in range(micros):
            first_load(m).start()

    for load in loads:
        load.start()

    barrier = pltpu.get_barrier_semaphore()

    def greet(where):
        pl.semaphore_signal(barrier, inc=1, device_id=where, device_id_type=MESH)

    for d in range(1, n_e):
        greet({"expert": peer_e(d)})
    for da in range(1, n_a):
        greet({"tensor": rank_of(da, 0)})
    for dc in range(1, pair):
        greet({"tensor": rank_of(0, dc)})

    @pl.when(p > 0)
    def _():
        greet({"pipe": p - 1})

    @pl.when(p < n_p - 1)
    def _():
        greet({"pipe": p + 1})

    toks = h_in.shape[1]
    quarter = toks // n_t
    down = lax.broadcasted_iota(jnp.int32, (toks, toks), 0)
    across = lax.broadcasted_iota(jnp.int32, (toks, toks), 1)
    same = down == across

    def column(row):
        return jnp.sum(jnp.where(same, row, jnp.zeros_like(row)), axis=1, keepdims=True)

    def row_of(col):
        return jnp.sum(jnp.where(same, col, jnp.zeros_like(col)), axis=0, keepdims=True)

    def slots(m):
        pos = jnp.sum(jnp.where(picks[m] == down, across, 0), axis=1, keepdims=True)
        pos_row = row_of(pos)
        block = lax.div(pos, quarter)
        before = (lax.div(pos_row, quarter) == block) & (pos_row < pos)
        found = []
        for e in range(n_e):
            named = jnp.zeros((1, toks), jnp.int32)
            for k in range(ids.shape[1]):
                named = named + jnp.where(ids[m, k:k + 1] == e, 1, 0)
            slot = jnp.sum(jnp.where(before, named, 0), axis=1, keepdims=True)
            kept = (column(named) > 0) & (slot < capacity)
            found.append(jnp.where(kept, block * capacity + slot, -1))
        return found

    def place(m):
        places = lax.broadcasted_iota(jnp.int32, (rows_ge, toks), 0)
        for e, target in enumerate(slots(m)):
            placing[m, e] = jnp.where(places == row_of(target), 1.0, 0.0).astype(BF16)
            w_row = jnp.zeros((1, toks), F32)
            for k in range(ids.shape[1]):
                w_row = w_row + jnp.where(ids[m, k:k + 1] == e, weights[m, k:k + 1], 0.0)
            spread = lax.broadcasted_iota(jnp.int32, (toks, rows_ge), 1) == target
            w_col = jnp.where(spread, column(w_row), 0.0)
            high = w_col.astype(BF16)
            comb[m, e, :toks] = high
            comb[m, e, toks:] = (w_col - high.astype(F32)).astype(BF16)

    for m in range(micros):
        place(m)

    ends = jnp.where(p > 0, 1, 0) + jnp.where(p < n_p - 1, 1, 0)
    pl.semaphore_wait(barrier, n_e - 1 + n_a - 1 + pair - 1 + ends)

    def relay(m):
        return remote(fresh.at[m], h_in.at[m], h_send.at[m], h_recv.at[m],
                      {"pipe": jnp.minimum(p + 1, n_p - 1)})

    def d_copy(m, d):
        return remote(send.at[m, d], x.at[m, r, z], d_send.at[m, d], d_recv.at[m, d],
                      {"expert": peer_e(d)})

    def f_copy(m, d, da):
        block = x.at[m, r, peer_e(n_e - d)]
        return remote(block, block, f_send.at[m, d, da], f_recv.at[m, d, da],
                      {"tensor": rank_of(da, 0)})

    def c_copy(m, d, da):
        block = x.at[m, rank_of(da, 0), peer_e(n_e - d)]
        return remote(block, block, c_send.at[m, d, da], c_recv.at[m, d, da],
                      {"tensor": rank_of(0, 1)})

    def p_copy(m, h, da):
        return remote(p_send.at[m, h, da], p_recv.at[m, h, da], ps_sem.at[m, h, da],
                      pr_sem.at[m, h, da], {"tensor": rank_of(0, 1)})

    def y_copy(m, d, da):
        return remote(y_send.at[m, d, da], y_recv.at[m, d, da], ys_sem.at[m, d, da],
                      yr_sem.at[m, d, da], {"tensor": rank_of(da, 0)})

    def z_copy(m, d):
        return remote(z_send.at[m, d], ret.at[m, z], zs_sem.at[m, d], zr_sem.at[m, d],
                      {"expert": peer_e(n_e - d)})

    def dispatch(m):
        @pl.when(p == 0)
        def _():
            first_load(m).wait()

        @pl.when(p > 0)
        def _():
            relay(m).wait_recv()

        h = h_in[m]
        for d in range(n_e - 1, -1, -1):
            block = jnp.dot(placing[m, peer_e(d)], h, preferred_element_type=F32).astype(BF16)
            if d:
                send[m, d] = block
                d_copy(m, d).start()
            else:
                x[m, r, z] = block

    def forward(m, d):
        if d:
            d_copy(m, d).wait_recv()
        for da in range(1, n_a):
            f_copy(m, d, da).start()
        if pair > 1:
            c_copy(m, d, 0).start()

    def pass_on(m, d):
        for da in range(1, n_a):
            f_copy(m, d, da).wait_recv()
            if pair > 1:
                c_copy(m, d, da).start()

    def compute(m, h):
        if m == 0 and h == 0:
            for load in loads:
                load.wait()
        if pair > 1:
            for d in halves[h]:
                for da in range(n_a):
                    c_copy(m, d, da).wait_recv()
        homes = [peer_e(n_e - d) for d in halves[h]]

        def rows_of(q):
            return jnp.concatenate([x[m, q, g].astype(F32) for g in homes], axis=0)

        ss = jnp.zeros((len(homes) * rows_ge, 1), F32)
        for q in range(n_t):
            xf = rows_of(q)
            ss = ss + jnp.sum(xf * xf, axis=-1, keepdims=True)
        inv = lax.rsqrt(ss * (1.0 / (n_t * width)) + epsilon)
        for q in range(n_t):
            cols = slice(q * width, (q + 1) * width)
            nq = (rows_of(q) * inv * gains[0:1, cols]).astype(BF16)
            gq = jnp.dot(nq, wg[cols, :], preferred_element_type=F32)
            uq = jnp.dot(nq, wu[cols, :], preferred_element_type=F32)
            if q == 0:
                g_acc[...] = gq
                u_acc[...] = uq
            else:
                g_acc[...] += gq
                u_acc[...] += uq
        gate = g_acc[...]
        hidden = (gate / (1.0 + jnp.exp(-gate)) * u_acc[...]).astype(BF16)
        for dc in list(range(1, pair)) + [0]:
            for da in list(range(1, n_a)) + [0]:
                start = pl.multiple_of(rank_of(da, dc) * width, width)
                part = jnp.dot(hidden, wd[:, pl.ds(start, width)], preferred_element_type=F32)
                if dc:
                    p_send[m, h, da] = part.astype(BF16)
                    p_copy(m, h, da).start()
                else:
                    own[m, h, da] = part.astype(BF16)

    def reduce_pair(m, h):
        for da in list(range(1, n_a)) + [0]:
            if pair > 1:
                p_copy(m, h, da).wait_recv()
            for i, d in enumerate(halves[h]):
                part = slice(i * rows_ge, (i + 1) * rows_ge)
                total = own[m, h, da, part].astype(F32)
                if pair > 1:
                    total = total + p_recv[m, h, da, part].astype(F32)
                y_send[m, d, da] = total.astype(BF16)
                if da:
                    y_copy(m, d, da).start()

    def reduce_far(m, d):
        total = y_send[m, d, 0].astype(F32)
        for da in range(1, n_a):
            y_copy(m, d, da).wait_recv()
            total = total + y_recv[m, d, da].astype(F32)
        if d:
            z_send[m, d] = total.astype(BF16)
            z_copy(m, d).start()
        else:
            ret[m, z] = total.astype(BF16)

    def combine(m):
        for d in range(n_e):
            e = peer_e(d)
            if d:
                z_copy(m, d).wait_recv()
            both = jnp.dot(comb[m, e], ret[m, e], preferred_element_type=F32)
            g_part = both[:toks] + both[toks:]
            update = g_part if d == 0 else update + g_part
        new = (h_in[m].astype(F32) + update).astype(BF16)
        fresh[m] = new
        out[0, m] = new

        @pl.when(p < n_p - 1)
        def _():
            relay(m).start()

    first, second = halves

    def step(fn, *args):
        return functools.partial(fn, *args)

    def head(m):
        steps = [step(forward, m, 0), step(forward, m, first[0]), step(pass_on, m, 0)]
        steps += [step(forward, m, d) for d in first[1:]]
        steps += [step(pass_on, m, d) for d in first]
        return steps

    def middle(m):
        steps = [step(compute, m, 0)]
        steps += [step(forward, m, d) for d in second[:-1]]
        steps += [step(reduce_pair, m, 0)]
        steps += [step(pass_on, m, d) for d in second[:-1]]
        return steps

    def back(m):
        return [step(compute, m, 1), step(reduce_pair, m, 1)]

    def tail(m):
        return [step(reduce_far, m, d) for d in first + second]

    def both_of(one, two):
        mixed = []
        for i in range(max(len(one), len(two))):
            mixed += one[i:i + 1] + two[i:i + 1]
        return mixed

    dispatch(0)

    @pl.when(p == 0)
    def _():
        for m in range(1, micros):
            dispatch(m)

    def late_dispatch(m):
        @pl.when(p > 0)
        def _():
            dispatch(m)

    plan = head(0)
    for m in range(micros):
        plan += middle(m)
        if m:
            plan += [step(combine, m - 1)]
        plan += back(m)
        if m + 1 < micros:
            plan += [step(late_dispatch, m + 1)]
            plan += both_of(tail(m), head(m + 1))
    plan += tail(micros - 1) + [step(combine, micros - 1)]
    for go in plan:
        go()

    for m in range(micros):
        for d in range(n_e):
            if d:
                d_copy(m, d).wait_send()
                z_copy(m, d).wait_send()
            for da in range(n_a):
                if da:
                    f_copy(m, d, da).wait_send()
                    y_copy(m, d, da).wait_send()
                if pair > 1:
                    c_copy(m, d, da).wait_send()
        if pair > 1:
            for h in range(len(halves)):
                for da in range(n_a):
                    p_copy(m, h, da).wait_send()

        @pl.when(p < n_p - 1)
        def _():
            relay(m).wait_send()


def local(mesh_shape, tokens, gains, route_ids, route_weights, picks, w_gate, w_up, w_down):
    n_p, n_t, n_e = mesh_shape
    micros, toks, model_width = tokens.shape
    route_count = route_ids.shape[3]
    quarter = toks // n_t
    capacity = 4 * quarter * route_count // (3 * n_e)
    width = model_width // n_t
    pair = 2 if n_t % 2 == 0 else 1
    n_a = n_t // pair
    rows_ge = -(-n_t * capacity // 8) * 8
    cut = (n_e + 1) // 2
    rows = cut * rows_ge
    hidden_width = w_gate.shape[3]

    ids = route_ids[0].transpose(0, 2, 1)
    weights = route_weights[0].transpose(0, 2, 1)
    order = picks[0]

    sizes = (micros, n_p, n_t, n_e, pair, rows_ge, width, capacity)
    dma = pltpu.SemaphoreType.DMA
    vmem = pl.BlockSpec(memory_space=pltpu.VMEM)
    anywhere = pl.BlockSpec(memory_space=pl.ANY)
    return pl.pallas_call(
        functools.partial(layer_kernel, sizes),
        out_shape=jax.ShapeDtypeStruct((1, micros, toks, width), BF16),
        in_specs=[anywhere, vmem, vmem, vmem, vmem, anywhere, anywhere, anywhere],
        out_specs=vmem,
        scratch_shapes=[
            pltpu.VMEM((micros, n_e, rows_ge, toks), BF16),
            pltpu.VMEM((micros, n_e, 2 * toks, rows_ge), BF16),
            pltpu.VMEM((micros, toks, width), BF16),
            pltpu.VMEM((micros, toks, width), BF16),
            pltpu.VMEM((micros, n_e, rows_ge, width), BF16),
            pltpu.VMEM((micros, n_t, n_e, rows_ge, width), BF16),
            pltpu.VMEM(w_gate.shape[2:], BF16),
            pltpu.VMEM(w_up.shape[2:], BF16),
            pltpu.VMEM(w_down.shape[2:], BF16),
            pltpu.VMEM((rows, hidden_width), F32),
            pltpu.VMEM((rows, hidden_width), F32),
            pltpu.VMEM((micros, 2, n_a, rows, width), BF16),
            pltpu.VMEM((micros, 2, n_a, rows, width), BF16),
            pltpu.VMEM((micros, 2, n_a, rows, width), BF16),
            pltpu.VMEM((micros, n_e, n_a, rows_ge, width), BF16),
            pltpu.VMEM((micros, n_e, n_a, rows_ge, width), BF16),
            pltpu.VMEM((micros, n_e, rows_ge, width), BF16),
            pltpu.VMEM((micros, n_e, rows_ge, width), BF16),
            dma((3,)), dma((micros,)), dma((micros,)), dma((micros,)),
            dma((micros, n_e)), dma((micros, n_e)),
            dma((micros, n_e, n_a)), dma((micros, n_e, n_a)),
            dma((micros, n_e, n_a)), dma((micros, n_e, n_a)),
            dma((micros, 2, n_a)), dma((micros, 2, n_a)),
            dma((micros, n_e, n_a)), dma((micros, n_e, n_a)),
            dma((micros, n_e)), dma((micros, n_e)),
        ],
        compiler_params=pltpu.CompilerParams(
            collective_id=0, has_side_effects=True, vmem_limit_bytes=67043328 - 600 * 1024
        ),
    )(tokens, gains, ids, weights, order, w_gate, w_up, w_down)


def solution(mesh):
    mesh_shape = (mesh.shape["pipe"], mesh.shape["tensor"], mesh.shape["expert"])
    return jax.shard_map(
        functools.partial(local, mesh_shape),
        mesh=mesh,
        in_specs=(
            P(None, "expert", None),
            P("pipe", None),
            P("pipe", None, "expert", None),
            P("pipe", None, "expert", None),
            P("pipe", None, "expert", None),
            P("pipe", "expert", None, "tensor"),
            P("pipe", "expert", None, "tensor"),
            P("pipe", "expert", "tensor", None),
        ),
        out_specs=P("pipe", None, "expert", "tensor"),
        check_vma=False,
    )
```

```python
import functools

import jax
import jax.numpy as jnp
from jax import lax
from jax.experimental import pallas as pl
from jax.experimental.pallas import tpu as pltpu
from jax.sharding import PartitionSpec as P

epsilon = 1e-06
MESH = pl.DeviceIdType.MESH
F32 = jnp.float32
BF16 = jnp.bfloat16


def layer_kernel(
    sizes, tokens, gains, ids, weights, picks, w_gate, w_up, w_down, out,
    placing, comb, h_in, fresh, send, x, wg, wu, wd, g_acc, u_acc, own, p_send, p_recv,
    y_send, y_recv, z_send, ret,
    w_sem, h_loc, h_send, h_recv, d_send, d_recv, f_send, f_recv, c_send, c_recv,
    ps_sem, pr_sem, ys_sem, yr_sem, zs_sem, zr_sem,
):
    micros, n_p, n_t, n_e, pair, rows_ge, width, capacity = sizes
    n_a = n_t // pair
    cut = (n_e + 1) // 2
    halves = [list(range(cut)), list(range(n_e - 1, cut - 1, -1))]
    p = lax.axis_index("pipe")
    r = lax.axis_index("tensor")
    z = lax.axis_index("expert")
    a = lax.div(r, pair)
    c = lax.rem(r, pair)

    def peer_e(d):
        other = z
        for bit in range(n_e.bit_length()):
            one = 1 << bit
            if d & one:
                other = other + one * (1 - 2 * lax.rem(lax.div(z, one), 2))
        return other

    def rank_of(da, dc):
        return lax.rem(a + da, n_a) * pair + lax.rem(c + dc, pair)

    def remote(src, dst, ssem, rsem, where):
        return pltpu.make_async_remote_copy(
            src_ref=src, dst_ref=dst, send_sem=ssem, recv_sem=rsem,
            device_id=where, device_id_type=MESH,
        )

    loads = [
        pltpu.make_async_copy(w_gate.at[0, 0], wg, w_sem.at[0]),
        pltpu.make_async_copy(w_up.at[0, 0], wu, w_sem.at[1]),
        pltpu.make_async_copy(w_down.at[0, 0], wd, w_sem.at[2]),
    ]

    def first_load(m):
        cols = pl.ds(pl.multiple_of(r * width, width), width)
        return pltpu.make_async_copy(tokens.at[m, :, cols], h_in.at[m], h_loc.at[m])

    @pl.when(p == 0)
    def _():
        for m in range(micros):
            first_load(m).start()

    for load in loads:
        load.start()

    barrier = pltpu.get_barrier_semaphore()

    def greet(where):
        pl.semaphore_signal(barrier, inc=1, device_id=where, device_id_type=MESH)

    for d in range(1, n_e):
        greet({"expert": peer_e(d)})
    for da in range(1, n_a):
        greet({"tensor": rank_of(da, 0)})
    for dc in range(1, pair):
        greet({"tensor": rank_of(0, dc)})

    @pl.when(p > 0)
    def _():
        greet({"pipe": p - 1})

    @pl.when(p < n_p - 1)
    def _():
        greet({"pipe": p + 1})

    toks = h_in.shape[1]
    quarter = toks // n_t
    down = lax.broadcasted_iota(jnp.int32, (toks, toks), 0)
    across = lax.broadcasted_iota(jnp.int32, (toks, toks), 1)
    same = down == across

    def column(row):
        return jnp.sum(jnp.where(same, row, jnp.zeros_like(row)), axis=1, keepdims=True)

    def row_of(col):
        return jnp.sum(jnp.where(same, col, jnp.zeros_like(col)), axis=0, keepdims=True)

    def slots(m):
        pos = jnp.sum(jnp.where(picks[m] == down, across, 0), axis=1, keepdims=True)
        pos_row = row_of(pos)
        block = lax.div(pos, quarter)
        before = (lax.div(pos_row, quarter) == block) & (pos_row < pos)
        found = []
        for e in range(n_e):
            named = jnp.zeros((1, toks), jnp.int32)
            for k in range(ids.shape[1]):
                named = named + jnp.where(ids[m, k:k + 1] == e, 1, 0)
            slot = jnp.sum(jnp.where(before, named, 0), axis=1, keepdims=True)
            kept = (column(named) > 0) & (slot < capacity)
            found.append(jnp.where(kept, block * capacity + slot, -1))
        return found

    def place(m):
        places = lax.broadcasted_iota(jnp.int32, (rows_ge, toks), 0)
        for e, target in enumerate(slots(m)):
            placing[m, e] = jnp.where(places == row_of(target), 1.0, 0.0).astype(BF16)
            w_row = jnp.zeros((1, toks), F32)
            for k in range(ids.shape[1]):
                w_row = w_row + jnp.where(ids[m, k:k + 1] == e, weights[m, k:k + 1], 0.0)
            spread = lax.broadcasted_iota(jnp.int32, (toks, rows_ge), 1) == target
            w_col = jnp.where(spread, column(w_row), 0.0)
            high = w_col.astype(BF16)
            comb[m, e, :toks] = high
            comb[m, e, toks:] = (w_col - high.astype(F32)).astype(BF16)

    for m in range(micros):
        place(m)

    ends = jnp.where(p > 0, 1, 0) + jnp.where(p < n_p - 1, 1, 0)
    pl.semaphore_wait(barrier, n_e - 1 + n_a - 1 + pair - 1 + ends)

    def relay(m):
        return remote(fresh.at[m], h_in.at[m], h_send.at[m], h_recv.at[m],
                      {"pipe": jnp.minimum(p + 1, n_p - 1)})

    def d_copy(m, d):
        return remote(send.at[m, d], x.at[m, r, z], d_send.at[m, d], d_recv.at[m, d],
                      {"expert": peer_e(d)})

    def f_copy(m, d, da):
        block = x.at[m, r, peer_e(d)]
        return remote(block, block, f_send.at[m, d, da], f_recv.at[m, d, da],
                      {"tensor": rank_of(da, 0)})

    def c_copy(m, d, da):
        block = x.at[m, rank_of(da, 0), peer_e(d)]
        return remote(block, block, c_send.at[m, d, da], c_recv.at[m, d, da],
                      {"tensor": rank_of(0, 1)})

    def p_copy(m, h, da):
        return remote(p_send.at[m, h, da], p_recv.at[m, h, da], ps_sem.at[m, h, da],
                      pr_sem.at[m, h, da], {"tensor": rank_of(0, 1)})

    def y_copy(m, d, da):
        return remote(y_send.at[m, d, da], y_recv.at[m, d, da], ys_sem.at[m, d, da],
                      yr_sem.at[m, d, da], {"tensor": rank_of(da, 0)})

    def z_copy(m, d):
        return remote(z_send.at[m, d], ret.at[m, z], zs_sem.at[m, d], zr_sem.at[m, d],
                      {"expert": peer_e(d)})

    def dispatch(m):
        @pl.when(p == 0)
        def _():
            first_load(m).wait()

        @pl.when(p > 0)
        def _():
            relay(m).wait_recv()

        h = h_in[m]
        for d in halves[0][1:] + halves[1] + [0]:
            block = jnp.dot(placing[m, peer_e(d)], h, preferred_element_type=F32).astype(BF16)
            if d:
                send[m, d] = block
                d_copy(m, d).start()
            else:
                x[m, r, z] = block

    def forward(m, d):
        if d:
            d_copy(m, d).wait_recv()
        for da in range(1, n_a):
            f_copy(m, d, da).start()
        if pair > 1:
            c_copy(m, d, 0).start()

    def pass_on(m, d):
        for da in range(1, n_a):
            f_copy(m, d, da).wait_recv()
            if pair > 1:
                c_copy(m, d, da).start()

    def compute(m, h):
        if m == 0 and h == 0:
            for load in loads:
                load.wait()
        if pair > 1:
            for d in halves[h]:
                for da in range(n_a):
                    c_copy(m, d, da).wait_recv()
        homes = [peer_e(d) for d in halves[h]]

        def rows_of(q):
            return jnp.concatenate([x[m, q, g].astype(F32) for g in homes], axis=0)

        ss = jnp.zeros((len(homes) * rows_ge, 1), F32)
        for q in range(n_t):
            xf = rows_of(q)
            ss = ss + jnp.sum(xf * xf, axis=-1, keepdims=True)
        inv = lax.rsqrt(ss * (1.0 / (n_t * width)) + epsilon)
        for q in range(n_t):
            cols = slice(q * width, (q + 1) * width)
            nq = (rows_of(q) * inv * gains[0:1, cols]).astype(BF16)
            gq = jnp.dot(nq, wg[cols, :], preferred_element_type=F32)
            uq = jnp.dot(nq, wu[cols, :], preferred_element_type=F32)
            if q == 0:
                g_acc[...] = gq
                u_acc[...] = uq
            else:
                g_acc[...] += gq
                u_acc[...] += uq
        gate = g_acc[...]
        hidden = (gate / (1.0 + jnp.exp(-gate)) * u_acc[...]).astype(BF16)
        for dc in list(range(1, pair)) + [0]:
            for da in list(range(1, n_a)) + [0]:
                start = pl.multiple_of(rank_of(da, dc) * width, width)
                part = jnp.dot(hidden, wd[:, pl.ds(start, width)], preferred_element_type=F32)
                if dc:
                    p_send[m, h, da] = part.astype(BF16)
                    p_copy(m, h, da).start()
                else:
                    own[m, h, da] = part.astype(BF16)

    def reduce_pair(m, h):
        for da in list(range(1, n_a)) + [0]:
            if pair > 1:
                p_copy(m, h, da).wait_recv()
            for i, d in enumerate(halves[h]):
                part = slice(i * rows_ge, (i + 1) * rows_ge)
                total = own[m, h, da, part].astype(F32)
                if pair > 1:
                    total = total + p_recv[m, h, da, part].astype(F32)
                y_send[m, d, da] = total.astype(BF16)
                if da:
                    y_copy(m, d, da).start()

    def reduce_far(m, d):
        total = y_send[m, d, 0].astype(F32)
        for da in range(1, n_a):
            y_copy(m, d, da).wait_recv()
            total = total + y_recv[m, d, da].astype(F32)
        if d:
            z_send[m, d] = total.astype(BF16)
            z_copy(m, d).start()
        else:
            ret[m, z] = total.astype(BF16)

    def combine(m):
        for d in range(n_e):
            e = peer_e(d)
            if d:
                z_copy(m, d).wait_recv()
            both = jnp.dot(comb[m, e], ret[m, e], preferred_element_type=F32)
            g_part = both[:toks] + both[toks:]
            update = g_part if d == 0 else update + g_part
        new = (h_in[m].astype(F32) + update).astype(BF16)
        fresh[m] = new
        out[0, m] = new

        @pl.when(p < n_p - 1)
        def _():
            relay(m).start()

    first, second = halves

    def step(fn, *args):
        return functools.partial(fn, *args)

    def when(test, fn, *args):
        pl.when(test)(functools.partial(fn, *args))

    def head(m):
        steps = [step(forward, m, d) for d in first]
        steps += [step(pass_on, m, d) for d in first[:-1]]
        steps += [step(forward, m, second[0]), step(pass_on, m, first[-1])]
        if m:
            steps += [step(when, p == 0, forward, m, d) for d in second[1:]]
        return steps

    def middle(m):
        steps = [step(compute, m, 0)]
        if m:
            steps += [step(when, p > 0, forward, m, d) for d in second[1:]]
        else:
            steps += [step(forward, m, d) for d in second[1:]]
        steps += [step(pass_on, m, d) for d in second[:-1]]
        steps += [step(reduce_pair, m, 0), step(pass_on, m, second[-1])]
        return steps

    def back(m):
        return [step(compute, m, 1), step(reduce_pair, m, 1)]

    def tail(m):
        return [step(reduce_far, m, d) for d in first[1:] + first[:1] + second]

    def both_of(one, two):
        mixed = []
        for i in range(max(len(one), len(two))):
            mixed += one[i:i + 1] + two[i:i + 1]
        return mixed

    dispatch(0)

    @pl.when(p == 0)
    def _():
        for m in range(1, micros):
            dispatch(m)

    def late_dispatch(m):
        @pl.when(p > 0)
        def _():
            dispatch(m)

    plan = head(0)
    for m in range(micros):
        plan += middle(m)
        if m:
            plan += [step(when, p < n_p - 1, combine, m - 1)]
        plan += back(m)
        if m + 1 < micros:
            plan += [step(late_dispatch, m + 1)]
            plan += both_of(tail(m), head(m + 1))
    plan += tail(micros - 1)
    plan += [step(when, p == n_p - 1, combine, m) for m in range(micros - 1)]
    plan += [step(combine, micros - 1)]
    for go in plan:
        go()

    for m in range(micros):
        for d in range(n_e):
            if d:
                d_copy(m, d).wait_send()
                z_copy(m, d).wait_send()
            for da in range(n_a):
                if da:
                    f_copy(m, d, da).wait_send()
                    y_copy(m, d, da).wait_send()
                if pair > 1:
                    c_copy(m, d, da).wait_send()
        if pair > 1:
            for h in range(len(halves)):
                for da in range(n_a):
                    p_copy(m, h, da).wait_send()

        @pl.when(p < n_p - 1)
        def _():
            relay(m).wait_send()


def local(mesh_shape, tokens, gains, route_ids, route_weights, picks, w_gate, w_up, w_down):
    n_p, n_t, n_e = mesh_shape
    micros, toks, model_width = tokens.shape
    route_count = route_ids.shape[3]
    quarter = toks // n_t
    capacity = 4 * quarter * route_count // (3 * n_e)
    width = model_width // n_t
    pair = 2 if n_t % 2 == 0 else 1
    n_a = n_t // pair
    rows_ge = -(-n_t * capacity // 8) * 8
    cut = (n_e + 1) // 2
    rows = cut * rows_ge
    hidden_width = w_gate.shape[3]

    ids = route_ids[0].transpose(0, 2, 1)
    weights = route_weights[0].transpose(0, 2, 1)
    order = picks[0]

    sizes = (micros, n_p, n_t, n_e, pair, rows_ge, width, capacity)
    dma = pltpu.SemaphoreType.DMA
    vmem = pl.BlockSpec(memory_space=pltpu.VMEM)
    anywhere = pl.BlockSpec(memory_space=pl.ANY)
    return pl.pallas_call(
        functools.partial(layer_kernel, sizes),
        out_shape=jax.ShapeDtypeStruct((1, micros, toks, width), BF16),
        in_specs=[anywhere, vmem, vmem, vmem, vmem, anywhere, anywhere, anywhere],
        out_specs=vmem,
        scratch_shapes=[
            pltpu.VMEM((micros, n_e, rows_ge, toks), BF16),
            pltpu.VMEM((micros, n_e, 2 * toks, rows_ge), BF16),
            pltpu.VMEM((micros, toks, width), BF16),
            pltpu.VMEM((micros, toks, width), BF16),
            pltpu.VMEM((micros, n_e, rows_ge, width), BF16),
            pltpu.VMEM((micros, n_t, n_e, rows_ge, width), BF16),
            pltpu.VMEM(w_gate.shape[2:], BF16),
            pltpu.VMEM(w_up.shape[2:], BF16),
            pltpu.VMEM(w_down.shape[2:], BF16),
            pltpu.VMEM((rows, hidden_width), F32),
            pltpu.VMEM((rows, hidden_width), F32),
            pltpu.VMEM((micros, 2, n_a, rows, width), BF16),
            pltpu.VMEM((micros, 2, n_a, rows, width), BF16),
            pltpu.VMEM((micros, 2, n_a, rows, width), BF16),
            pltpu.VMEM((micros, n_e, n_a, rows_ge, width), BF16),
            pltpu.VMEM((micros, n_e, n_a, rows_ge, width), BF16),
            pltpu.VMEM((micros, n_e, rows_ge, width), BF16),
            pltpu.VMEM((micros, n_e, rows_ge, width), BF16),
            dma((3,)), dma((micros,)), dma((micros,)), dma((micros,)),
            dma((micros, n_e)), dma((micros, n_e)),
            dma((micros, n_e, n_a)), dma((micros, n_e, n_a)),
            dma((micros, n_e, n_a)), dma((micros, n_e, n_a)),
            dma((micros, 2, n_a)), dma((micros, 2, n_a)),
            dma((micros, n_e, n_a)), dma((micros, n_e, n_a)),
            dma((micros, n_e)), dma((micros, n_e)),
        ],
        compiler_params=pltpu.CompilerParams(
            collective_id=0, has_side_effects=True, vmem_limit_bytes=67043328 - 600 * 1024
        ),
    )(tokens, gains, ids, weights, order, w_gate, w_up, w_down)


def solution(mesh):
    mesh_shape = (mesh.shape["pipe"], mesh.shape["tensor"], mesh.shape["expert"])
    return jax.shard_map(
        functools.partial(local, mesh_shape),
        mesh=mesh,
        in_specs=(
            P(None, "expert", None),
            P("pipe", None),
            P("pipe", None, "expert", None),
            P("pipe", None, "expert", None),
            P("pipe", None, "expert", None),
            P("pipe", "expert", None, "tensor"),
            P("pipe", "expert", None, "tensor"),
            P("pipe", "expert", "tensor", None),
        ),
        out_specs=P("pipe", None, "expert", "tensor"),
        check_vma=False,
    )
```

```python
import functools

import jax
import jax.numpy as jnp
from jax import lax
from jax.experimental import pallas as pl
from jax.experimental.pallas import tpu as pltpu
from jax.sharding import PartitionSpec as P

epsilon = 1e-06
MESH = pl.DeviceIdType.MESH
F32 = jnp.float32
BF16 = jnp.bfloat16


def layer_kernel(
    sizes, tokens, gains, ids, weights, picks, w_gate, w_up, w_down, out,
    placing, comb, h_in, fresh, send, x, wg, wu, wd, g_acc, u_acc, own, p_send, p_recv,
    y_send, y_recv, z_send, ret,
    w_sem, h_loc, h_send, h_recv, d_send, d_recv, f_send, f_recv, c_send, c_recv,
    ps_sem, pr_sem, ys_sem, yr_sem, zs_sem, zr_sem,
):
    micros, n_p, n_t, n_e, pair, rows_ge, width, capacity = sizes
    n_a = n_t // pair
    cut = (n_e + 1) // 2
    halves = [list(range(cut)), list(range(n_e - 1, cut - 1, -1))]
    p = lax.axis_index("pipe")
    r = lax.axis_index("tensor")
    z = lax.axis_index("expert")
    a = lax.div(r, pair)
    c = lax.rem(r, pair)

    def peer_e(d):
        other = z
        for bit in range(n_e.bit_length()):
            one = 1 << bit
            if d & one:
                other = other + one * (1 - 2 * lax.rem(lax.div(z, one), 2))
        return other

    def rank_of(da, dc):
        return lax.rem(a + da, n_a) * pair + lax.rem(c + dc, pair)

    def remote(src, dst, ssem, rsem, where):
        return pltpu.make_async_remote_copy(
            src_ref=src, dst_ref=dst, send_sem=ssem, recv_sem=rsem,
            device_id=where, device_id_type=MESH,
        )

    loads = [
        pltpu.make_async_copy(w_gate.at[0, 0], wg, w_sem.at[0]),
        pltpu.make_async_copy(w_up.at[0, 0], wu, w_sem.at[1]),
        pltpu.make_async_copy(w_down.at[0, 0], wd, w_sem.at[2]),
    ]

    def first_load(m):
        cols = pl.ds(pl.multiple_of(r * width, width), width)
        return pltpu.make_async_copy(tokens.at[m, :, cols], h_in.at[m], h_loc.at[m])

    @pl.when(p == 0)
    def _():
        for m in range(micros):
            first_load(m).start()

    for load in loads:
        load.start()

    barrier = pltpu.get_barrier_semaphore()

    def greet(where):
        pl.semaphore_signal(barrier, inc=1, device_id=where, device_id_type=MESH)

    for d in range(1, n_e):
        greet({"expert": peer_e(d)})
    for da in range(1, n_a):
        greet({"tensor": rank_of(da, 0)})
    for dc in range(1, pair):
        greet({"tensor": rank_of(0, dc)})

    @pl.when(p > 0)
    def _():
        greet({"pipe": p - 1})

    @pl.when(p < n_p - 1)
    def _():
        greet({"pipe": p + 1})

    toks = h_in.shape[1]
    quarter = toks // n_t
    down = lax.broadcasted_iota(jnp.int32, (toks, toks), 0)
    across = lax.broadcasted_iota(jnp.int32, (toks, toks), 1)
    same = down == across

    def column(row):
        return jnp.sum(jnp.where(same, row, jnp.zeros_like(row)), axis=1, keepdims=True)

    def row_of(col):
        return jnp.sum(jnp.where(same, col, jnp.zeros_like(col)), axis=0, keepdims=True)

    def slots(m):
        pos = jnp.sum(jnp.where(picks[m] == down, across, 0), axis=1, keepdims=True)
        pos_row = row_of(pos)
        block = lax.div(pos, quarter)
        before = (lax.div(pos_row, quarter) == block) & (pos_row < pos)
        found = []
        for e in range(n_e):
            named = jnp.zeros((1, toks), jnp.int32)
            for k in range(ids.shape[1]):
                named = named + jnp.where(ids[m, k:k + 1] == e, 1, 0)
            slot = jnp.sum(jnp.where(before, named, 0), axis=1, keepdims=True)
            kept = (column(named) > 0) & (slot < capacity)
            found.append(jnp.where(kept, block * capacity + slot, -1))
        return found

    def place(m, targets):
        places = lax.broadcasted_iota(jnp.int32, (rows_ge, toks), 0)
        for e, target in enumerate(targets):
            placing[m, e] = jnp.where(places == row_of(target), 1.0, 0.0).astype(BF16)

    def weigh(m, targets):
        for e, target in enumerate(targets):
            w_row = jnp.zeros((1, toks), F32)
            for k in range(ids.shape[1]):
                w_row = w_row + jnp.where(ids[m, k:k + 1] == e, weights[m, k:k + 1], 0.0)
            spread = lax.broadcasted_iota(jnp.int32, (toks, rows_ge), 1) == target
            w_col = jnp.where(spread, column(w_row), 0.0)
            high = w_col.astype(BF16)
            comb[m, e, :toks] = high
            comb[m, e, toks:] = (w_col - high.astype(F32)).astype(BF16)

    place(0, slots(0))

    ends = jnp.where(p > 0, 1, 0) + jnp.where(p < n_p - 1, 1, 0)
    pl.semaphore_wait(barrier, n_e - 1 + n_a - 1 + pair - 1 + ends)

    def relay(m):
        return remote(fresh.at[m], h_in.at[m], h_send.at[m], h_recv.at[m],
                      {"pipe": jnp.minimum(p + 1, n_p - 1)})

    def d_copy(m, d):
        return remote(send.at[m, d], x.at[m, r, z], d_send.at[m, d], d_recv.at[m, d],
                      {"expert": peer_e(d)})

    def f_copy(m, d, da):
        block = x.at[m, r, peer_e(d)]
        return remote(block, block, f_send.at[m, d, da], f_recv.at[m, d, da],
                      {"tensor": rank_of(da, 0)})

    def c_copy(m, d, da):
        block = x.at[m, rank_of(da, 0), peer_e(d)]
        return remote(block, block, c_send.at[m, d, da], c_recv.at[m, d, da],
                      {"tensor": rank_of(0, 1)})

    def p_copy(m, h, da):
        return remote(p_send.at[m, h, da], p_recv.at[m, h, da], ps_sem.at[m, h, da],
                      pr_sem.at[m, h, da], {"tensor": rank_of(0, 1)})

    def y_copy(m, d, da):
        return remote(y_send.at[m, d, da], y_recv.at[m, d, da], ys_sem.at[m, d, da],
                      yr_sem.at[m, d, da], {"tensor": rank_of(da, 0)})

    def z_copy(m, d):
        return remote(z_send.at[m, d], ret.at[m, z], zs_sem.at[m, d], zr_sem.at[m, d],
                      {"expert": peer_e(d)})

    def dispatch(m):
        @pl.when(p == 0)
        def _():
            first_load(m).wait()

        @pl.when(p > 0)
        def _():
            relay(m).wait_recv()

        h = h_in[m]
        for d in halves[0][1:] + halves[1] + [0]:
            block = jnp.dot(placing[m, peer_e(d)], h, preferred_element_type=F32).astype(BF16)
            if d:
                send[m, d] = block
                d_copy(m, d).start()
            else:
                x[m, r, z] = block

    def forward(m, d):
        if d:
            d_copy(m, d).wait_recv()
        for da in range(1, n_a):
            f_copy(m, d, da).start()
        if pair > 1:
            c_copy(m, d, 0).start()

    def pass_on(m, d):
        for da in range(1, n_a):
            f_copy(m, d, da).wait_recv()
            if pair > 1:
                c_copy(m, d, da).start()

    def compute(m, h):
        if m == 0 and h == 0:
            for load in loads:
                load.wait()
        if pair > 1:
            for d in halves[h]:
                for da in range(n_a):
                    c_copy(m, d, da).wait_recv()
        homes = [peer_e(d) for d in halves[h]]

        def rows_of(q):
            return jnp.concatenate([x[m, q, g].astype(F32) for g in homes], axis=0)

        ss = jnp.zeros((len(homes) * rows_ge, 1), F32)
        for q in range(n_t):
            xf = rows_of(q)
            ss = ss + jnp.sum(xf * xf, axis=-1, keepdims=True)
        inv = lax.rsqrt(ss * (1.0 / (n_t * width)) + epsilon)
        for q in range(n_t):
            cols = slice(q * width, (q + 1) * width)
            nq = (rows_of(q) * inv * gains[0:1, cols]).astype(BF16)
            gq = jnp.dot(nq, wg[cols, :], preferred_element_type=F32)
            uq = jnp.dot(nq, wu[cols, :], preferred_element_type=F32)
            if q == 0:
                g_acc[...] = gq
                u_acc[...] = uq
            else:
                g_acc[...] += gq
                u_acc[...] += uq
        gate = g_acc[...]
        hidden = (gate / (1.0 + jnp.exp(-gate)) * u_acc[...]).astype(BF16)
        for dc in list(range(1, pair)) + [0]:
            for da in list(range(1, n_a)) + [0]:
                start = pl.multiple_of(rank_of(da, dc) * width, width)
                part = jnp.dot(hidden, wd[:, pl.ds(start, width)], preferred_element_type=F32)
                if dc:
                    p_send[m, h, da] = part.astype(BF16)
                    p_copy(m, h, da).start()
                else:
                    own[m, h, da] = part.astype(BF16)

    def reduce_pair(m, h):
        for da in list(range(1, n_a)) + [0]:
            if pair > 1:
                p_copy(m, h, da).wait_recv()
            for i, d in enumerate(halves[h]):
                part = slice(i * rows_ge, (i + 1) * rows_ge)
                total = own[m, h, da, part].astype(F32)
                if pair > 1:
                    total = total + p_recv[m, h, da, part].astype(F32)
                y_send[m, d, da] = total.astype(BF16)
                if da and d:
                    y_copy(m, d, da).start()
            if h and da:
                y_copy(m, 0, da).start()

    def reduce_far(m, d):
        total = y_send[m, d, 0].astype(F32)
        for da in range(1, n_a):
            y_copy(m, d, da).wait_recv()
            total = total + y_recv[m, d, da].astype(F32)
        if d:
            z_send[m, d] = total.astype(BF16)
            z_copy(m, d).start()
        else:
            ret[m, z] = total.astype(BF16)

    def combine(m):
        for d in halves[0] + halves[1]:
            e = peer_e(d)
            if d:
                z_copy(m, d).wait_recv()
            both = jnp.dot(comb[m, e], ret[m, e], preferred_element_type=F32)
            g_part = both[:toks] + both[toks:]
            update = g_part if d == 0 else update + g_part
        new = (h_in[m].astype(F32) + update).astype(BF16)
        fresh[m] = new
        out[0, m] = new

        @pl.when(p < n_p - 1)
        def _():
            relay(m).start()

    first, second = halves

    def step(fn, *args):
        return functools.partial(fn, *args)

    def when(test, fn, *args):
        pl.when(test)(functools.partial(fn, *args))

    def head(m):
        steps = [step(forward, m, d) for d in first]
        steps += [step(pass_on, m, d) for d in first[:-1]]
        steps += [step(forward, m, second[0]), step(pass_on, m, first[-1])]
        if m:
            steps += [step(when, p == 0, forward, m, d) for d in second[1:]]
        return steps

    def middle(m):
        steps = [step(compute, m, 0)]
        if m:
            steps += [step(when, p > 0, forward, m, d) for d in second[1:]]
        else:
            steps += [step(forward, m, d) for d in second[1:]]
        steps += [step(pass_on, m, d) for d in second[:-1]]
        steps += [step(reduce_pair, m, 0), step(pass_on, m, second[-1])]
        return steps

    def back(m):
        return [step(compute, m, 1), step(reduce_pair, m, 1)]

    def tail(m):
        return [step(reduce_far, m, d) for d in first[1:] + second + first[:1]]

    def both_of(one, two):
        mixed = []
        for i in range(max(len(one), len(two))):
            mixed += one[i:i + 1] + two[i:i + 1]
        return mixed

    dispatch(0)
    head(0)[0]()
    for m in range(1, micros):
        place(m, slots(m))

    @pl.when(p == 0)
    def _():
        for m in range(1, micros):
            dispatch(m)

    for m in range(micros):
        weigh(m, slots(m))

    def late_dispatch(m):
        @pl.when(p > 0)
        def _():
            dispatch(m)

    plan = head(0)[1:]
    for m in range(micros):
        plan += middle(m)
        if m:
            plan += [step(when, p < n_p - 1, combine, m - 1)]
        plan += back(m)
        if m + 1 < micros:
            plan += [step(late_dispatch, m + 1)]
            plan += both_of(tail(m), head(m + 1))
    plan += tail(micros - 1)
    plan += [step(when, p == n_p - 1, combine, m) for m in range(micros - 1)]
    plan += [step(combine, micros - 1)]
    for go in plan:
        go()

    for m in range(micros):
        for d in range(n_e):
            if d:
                d_copy(m, d).wait_send()
                z_copy(m, d).wait_send()
            for da in range(n_a):
                if da:
                    f_copy(m, d, da).wait_send()
                    y_copy(m, d, da).wait_send()
                if pair > 1:
                    c_copy(m, d, da).wait_send()
        if pair > 1:
            for h in range(len(halves)):
                for da in range(n_a):
                    p_copy(m, h, da).wait_send()

        @pl.when(p < n_p - 1)
        def _():
            relay(m).wait_send()


def local(mesh_shape, tokens, gains, route_ids, route_weights, picks, w_gate, w_up, w_down):
    n_p, n_t, n_e = mesh_shape
    micros, toks, model_width = tokens.shape
    route_count = route_ids.shape[3]
    quarter = toks // n_t
    capacity = 4 * quarter * route_count // (3 * n_e)
    width = model_width // n_t
    pair = 2 if n_t % 2 == 0 else 1
    n_a = n_t // pair
    rows_ge = -(-n_t * capacity // 8) * 8
    cut = (n_e + 1) // 2
    rows = cut * rows_ge
    hidden_width = w_gate.shape[3]

    ids = route_ids[0].transpose(0, 2, 1)
    weights = route_weights[0].transpose(0, 2, 1)
    order = picks[0]

    sizes = (micros, n_p, n_t, n_e, pair, rows_ge, width, capacity)
    dma = pltpu.SemaphoreType.DMA
    vmem = pl.BlockSpec(memory_space=pltpu.VMEM)
    anywhere = pl.BlockSpec(memory_space=pl.ANY)
    return pl.pallas_call(
        functools.partial(layer_kernel, sizes),
        out_shape=jax.ShapeDtypeStruct((1, micros, toks, width), BF16),
        in_specs=[anywhere, vmem, vmem, vmem, vmem, anywhere, anywhere, anywhere],
        out_specs=vmem,
        scratch_shapes=[
            pltpu.VMEM((micros, n_e, rows_ge, toks), BF16),
            pltpu.VMEM((micros, n_e, 2 * toks, rows_ge), BF16),
            pltpu.VMEM((micros, toks, width), BF16),
            pltpu.VMEM((micros, toks, width), BF16),
            pltpu.VMEM((micros, n_e, rows_ge, width), BF16),
            pltpu.VMEM((micros, n_t, n_e, rows_ge, width), BF16),
            pltpu.VMEM(w_gate.shape[2:], BF16),
            pltpu.VMEM(w_up.shape[2:], BF16),
            pltpu.VMEM(w_down.shape[2:], BF16),
            pltpu.VMEM((rows, hidden_width), F32),
            pltpu.VMEM((rows, hidden_width), F32),
            pltpu.VMEM((micros, 2, n_a, rows, width), BF16),
            pltpu.VMEM((micros, 2, n_a, rows, width), BF16),
            pltpu.VMEM((micros, 2, n_a, rows, width), BF16),
            pltpu.VMEM((micros, n_e, n_a, rows_ge, width), BF16),
            pltpu.VMEM((micros, n_e, n_a, rows_ge, width), BF16),
            pltpu.VMEM((micros, n_e, rows_ge, width), BF16),
            pltpu.VMEM((micros, n_e, rows_ge, width), BF16),
            dma((3,)), dma((micros,)), dma((micros,)), dma((micros,)),
            dma((micros, n_e)), dma((micros, n_e)),
            dma((micros, n_e, n_a)), dma((micros, n_e, n_a)),
            dma((micros, n_e, n_a)), dma((micros, n_e, n_a)),
            dma((micros, 2, n_a)), dma((micros, 2, n_a)),
            dma((micros, n_e, n_a)), dma((micros, n_e, n_a)),
            dma((micros, n_e)), dma((micros, n_e)),
        ],
        compiler_params=pltpu.CompilerParams(
            collective_id=0, has_side_effects=True, vmem_limit_bytes=67043328 - 600 * 1024
        ),
    )(tokens, gains, ids, weights, order, w_gate, w_up, w_down)


def solution(mesh):
    mesh_shape = (mesh.shape["pipe"], mesh.shape["tensor"], mesh.shape["expert"])
    return jax.shard_map(
        functools.partial(local, mesh_shape),
        mesh=mesh,
        in_specs=(
            P(None, "expert", None),
            P("pipe", None),
            P("pipe", None, "expert", None),
            P("pipe", None, "expert", None),
            P("pipe", None, "expert", None),
            P("pipe", "expert", None, "tensor"),
            P("pipe", "expert", None, "tensor"),
            P("pipe", "expert", "tensor", None),
        ),
        out_specs=P("pipe", None, "expert", "tensor"),
        check_vma=False,
    )
```

```python
import functools

import jax
import jax.numpy as jnp
from jax import lax
from jax.experimental import pallas as pl
from jax.experimental.pallas import tpu as pltpu
from jax.sharding import PartitionSpec as P

epsilon = 1e-06
MESH = pl.DeviceIdType.MESH
F32 = jnp.float32
BF16 = jnp.bfloat16


def layer_kernel(
    sizes, tokens, gains_in, ids_in, weights_in, picks_in, w_gate, w_up, w_down, out,
    gains, ids, weights, picks, placing, comb, h_in, fresh, send, x, wg, wu, wd, g_acc, u_acc, own, p_send, p_recv,
    y_send, y_recv, z_send, ret,
    s_sem, w_sem, h_loc, h_send, h_recv, d_send, d_recv, f_send, f_recv, c_send, c_recv,
    ps_sem, pr_sem, ys_sem, yr_sem, zs_sem, zr_sem,
):
    micros, n_p, n_t, n_e, pair, rows_ge, width, capacity = sizes
    n_a = n_t // pair
    cut = (n_e + 1) // 2
    halves = [list(range(cut)), list(range(n_e - 1, cut - 1, -1))]
    p = lax.axis_index("pipe")
    r = lax.axis_index("tensor")
    z = lax.axis_index("expert")
    a = lax.div(r, pair)
    c = lax.rem(r, pair)

    def peer_e(d):
        other = z
        for bit in range(n_e.bit_length()):
            one = 1 << bit
            if d & one:
                other = other + one * (1 - 2 * lax.rem(lax.div(z, one), 2))
        return other

    def rank_of(da, dc):
        return lax.rem(a + da, n_a) * pair + lax.rem(c + dc, pair)

    def remote(src, dst, ssem, rsem, where):
        return pltpu.make_async_remote_copy(
            src_ref=src, dst_ref=dst, send_sem=ssem, recv_sem=rsem,
            device_id=where, device_id_type=MESH,
        )

    loads = [
        pltpu.make_async_copy(w_gate.at[0, 0], wg, w_sem.at[0]),
        pltpu.make_async_copy(w_up.at[0, 0], wu, w_sem.at[1]),
        pltpu.make_async_copy(w_down.at[0, 0], wd, w_sem.at[2]),
    ]

    def first_load(m):
        cols = pl.ds(pl.multiple_of(r * width, width), width)
        return pltpu.make_async_copy(tokens.at[m, :, cols], h_in.at[m], h_loc.at[m])

    small = [
        pltpu.make_async_copy(src, dst, s_sem.at[i])
        for i, (src, dst) in enumerate(
            [(picks_in, picks), (ids_in, ids), (weights_in, weights), (gains_in, gains)]
        )
    ]
    for load in small:
        load.start()

    @pl.when(p == 0)
    def _():
        for m in range(micros):
            first_load(m).start()

    for load in loads:
        load.start()

    barrier = pltpu.get_barrier_semaphore()

    def greet(where):
        pl.semaphore_signal(barrier, inc=1, device_id=where, device_id_type=MESH)

    for d in range(1, n_e):
        greet({"expert": peer_e(d)})
    for da in range(1, n_a):
        greet({"tensor": rank_of(da, 0)})
    for dc in range(1, pair):
        greet({"tensor": rank_of(0, dc)})

    @pl.when(p > 0)
    def _():
        greet({"pipe": p - 1})

    @pl.when(p < n_p - 1)
    def _():
        greet({"pipe": p + 1})

    toks = h_in.shape[1]
    quarter = toks // n_t
    down = lax.broadcasted_iota(jnp.int32, (toks, toks), 0)
    across = lax.broadcasted_iota(jnp.int32, (toks, toks), 1)
    same = down == across

    def column(row):
        return jnp.sum(jnp.where(same, row, jnp.zeros_like(row)), axis=1, keepdims=True)

    def row_of(col):
        return jnp.sum(jnp.where(same, col, jnp.zeros_like(col)), axis=0, keepdims=True)

    def slots(m):
        pos = jnp.sum(jnp.where(picks[m] == down, across, 0), axis=1, keepdims=True)
        pos_row = row_of(pos)
        block = lax.div(pos, quarter)
        before = (lax.div(pos_row, quarter) == block) & (pos_row < pos)
        found = []
        for e in range(n_e):
            named = jnp.zeros((1, toks), jnp.int32)
            for k in range(ids.shape[1]):
                named = named + jnp.where(ids[m, k:k + 1] == e, 1, 0)
            slot = jnp.sum(jnp.where(before, named, 0), axis=1, keepdims=True)
            kept = (column(named) > 0) & (slot < capacity)
            found.append(jnp.where(kept, block * capacity + slot, -1))
        return found

    def place(m, targets):
        places = lax.broadcasted_iota(jnp.int32, (rows_ge, toks), 0)
        for e, target in enumerate(targets):
            placing[m, e] = jnp.where(places == row_of(target), 1.0, 0.0).astype(BF16)

    def weigh(m):
        for e, target in enumerate(slots(m)):
            w_row = jnp.zeros((1, toks), F32)
            for k in range(ids.shape[1]):
                w_row = w_row + jnp.where(ids[m, k:k + 1] == e, weights[m, k:k + 1], 0.0)
            spread = lax.broadcasted_iota(jnp.int32, (toks, rows_ge), 1) == target
            w_col = jnp.where(spread, column(w_row), 0.0)
            high = w_col.astype(BF16)
            comb[m, e, :toks] = high
            comb[m, e, toks:] = (w_col - high.astype(F32)).astype(BF16)

    for load in small:
        load.wait()
    place(0, slots(0))

    ends = jnp.where(p > 0, 1, 0) + jnp.where(p < n_p - 1, 1, 0)
    pl.semaphore_wait(barrier, n_e - 1 + n_a - 1 + pair - 1 + ends)

    def relay(m):
        return remote(fresh.at[m], h_in.at[m], h_send.at[m], h_recv.at[m],
                      {"pipe": jnp.minimum(p + 1, n_p - 1)})

    def d_copy(m, d):
        return remote(send.at[m, d], x.at[m, r, z], d_send.at[m, d], d_recv.at[m, d],
                      {"expert": peer_e(d)})

    def f_copy(m, d, da):
        block = x.at[m, r, peer_e(d)]
        return remote(block, block, f_send.at[m, d, da], f_recv.at[m, d, da],
                      {"tensor": rank_of(da, 0)})

    def c_copy(m, d, da):
        block = x.at[m, rank_of(da, 0), peer_e(d)]
        return remote(block, block, c_send.at[m, d, da], c_recv.at[m, d, da],
                      {"tensor": rank_of(0, 1)})

    def p_copy(m, h, da):
        return remote(p_send.at[m, h, da], p_recv.at[m, h, da], ps_sem.at[m, h, da],
                      pr_sem.at[m, h, da], {"tensor": rank_of(0, 1)})

    def y_copy(m, d, da):
        return remote(y_send.at[m, d, da], y_recv.at[m, d, da], ys_sem.at[m, d, da],
                      yr_sem.at[m, d, da], {"tensor": rank_of(da, 0)})

    def z_copy(m, d):
        return remote(z_send.at[m, d], ret.at[m, z], zs_sem.at[m, d], zr_sem.at[m, d],
                      {"expert": peer_e(d)})

    def dispatch(m):
        @pl.when(p == 0)
        def _():
            first_load(m).wait()

        @pl.when(p > 0)
        def _():
            relay(m).wait_recv()

        h = h_in[m]
        for d in halves[0][1:] + halves[1] + [0]:
            block = jnp.dot(placing[m, peer_e(d)], h, preferred_element_type=F32).astype(BF16)
            if d:
                send[m, d] = block
                d_copy(m, d).start()
            else:
                x[m, r, z] = block

    def forward(m, d):
        if d:
            d_copy(m, d).wait_recv()
        for da in range(1, n_a):
            f_copy(m, d, da).start()
        if pair > 1:
            c_copy(m, d, 0).start()

    def pass_on(m, d):
        for da in range(1, n_a):
            f_copy(m, d, da).wait_recv()
            if pair > 1:
                c_copy(m, d, da).start()

    def compute(m, h):
        if m == 0 and h == 0:
            for load in loads:
                load.wait()
        if pair > 1:
            for d in halves[h]:
                for da in range(n_a):
                    c_copy(m, d, da).wait_recv()
        homes = [peer_e(d) for d in halves[h]]

        def rows_of(q):
            return jnp.concatenate([x[m, q, g].astype(F32) for g in homes], axis=0)

        ss = jnp.zeros((len(homes) * rows_ge, 1), F32)
        for q in range(n_t):
            xf = rows_of(q)
            ss = ss + jnp.sum(xf * xf, axis=-1, keepdims=True)
        inv = lax.rsqrt(ss * (1.0 / (n_t * width)) + epsilon)
        for q in range(n_t):
            cols = slice(q * width, (q + 1) * width)
            nq = (rows_of(q) * inv * gains[0:1, cols]).astype(BF16)
            gq = jnp.dot(nq, wg[cols, :], preferred_element_type=F32)
            uq = jnp.dot(nq, wu[cols, :], preferred_element_type=F32)
            if q == 0:
                g_acc[...] = gq
                u_acc[...] = uq
            else:
                g_acc[...] += gq
                u_acc[...] += uq
        gate = g_acc[...]
        hidden = (gate / (1.0 + jnp.exp(-gate)) * u_acc[...]).astype(BF16)
        for dc in list(range(1, pair)) + [0]:
            for da in list(range(1, n_a)) + [0]:
                start = pl.multiple_of(rank_of(da, dc) * width, width)
                part = jnp.dot(hidden, wd[:, pl.ds(start, width)], preferred_element_type=F32)
                if dc:
                    p_send[m, h, da] = part.astype(BF16)
                    p_copy(m, h, da).start()
                else:
                    own[m, h, da] = part.astype(BF16)

    def reduce_pair(m, h):
        for da in list(range(1, n_a)) + [0]:
            if pair > 1:
                p_copy(m, h, da).wait_recv()
            for i, d in reversed(list(enumerate(halves[h]))) if h == 0 else enumerate(halves[h]):
                part = slice(i * rows_ge, (i + 1) * rows_ge)
                total = own[m, h, da, part].astype(F32)
                if pair > 1:
                    total = total + p_recv[m, h, da, part].astype(F32)
                y_send[m, d, da] = total.astype(BF16)
                if da:
                    y_copy(m, d, da).start()

    def reduce_far(m, d):
        total = y_send[m, d, 0].astype(F32)
        for da in range(1, n_a):
            y_copy(m, d, da).wait_recv()
            total = total + y_recv[m, d, da].astype(F32)
        if d:
            z_send[m, d] = total.astype(BF16)
            z_copy(m, d).start()
        else:
            ret[m, z] = total.astype(BF16)

    def combine(m):
        for d in halves[0] + halves[1]:
            e = peer_e(d)
            if d:
                z_copy(m, d).wait_recv()
            both = jnp.dot(comb[m, e], ret[m, e], preferred_element_type=F32)
            g_part = both[:toks] + both[toks:]
            update = g_part if d == 0 else update + g_part
        new = (h_in[m].astype(F32) + update).astype(BF16)
        fresh[m] = new
        out[0, m] = new

        @pl.when(p < n_p - 1)
        def _():
            relay(m).start()

    first, second = halves

    def step(fn, *args):
        return functools.partial(fn, *args)

    def when(test, fn, *args):
        pl.when(test)(functools.partial(fn, *args))

    def head(m):
        steps = [step(forward, m, d) for d in first]
        steps += [step(pass_on, m, d) for d in first[:-1]]
        steps += [step(forward, m, second[0]), step(pass_on, m, first[-1])]
        if m:
            steps += [step(when, p == 0, forward, m, d) for d in second[1:]]
        return steps

    def middle(m):
        steps = [step(compute, m, 0)]
        if m:
            steps += [step(when, p > 0, forward, m, d) for d in second[1:]]
        else:
            steps += [step(forward, m, d) for d in second[1:]]
        steps += [step(pass_on, m, d) for d in second[:-1]]
        steps += [step(reduce_pair, m, 0), step(weigh, m), step(pass_on, m, second[-1])]
        return steps

    def back(m):
        return [step(compute, m, 1), step(reduce_pair, m, 1)]

    def tail(m):
        return [step(reduce_far, m, d) for d in first[1:] + first[:1] + second]

    def both_of(one, two):
        mixed = []
        for i in range(max(len(one), len(two))):
            mixed += one[i:i + 1] + two[i:i + 1]
        return mixed

    dispatch(0)
    head(0)[0]()
    for m in range(1, micros):
        place(m, slots(m))

    @pl.when(p == 0)
    def _():
        for m in range(1, micros):
            dispatch(m)

    def late_dispatch(m):
        @pl.when(p > 0)
        def _():
            dispatch(m)

    plan = head(0)[1:]
    for m in range(micros):
        plan += middle(m)
        if m:
            plan += [step(when, p < n_p - 1, combine, m - 1)]
        plan += back(m)
        if m + 1 < micros:
            plan += [step(late_dispatch, m + 1)]
            plan += both_of(tail(m), head(m + 1))
    plan += tail(micros - 1)
    plan += [step(when, p == n_p - 1, combine, m) for m in range(micros - 1)]
    plan += [step(combine, micros - 1)]
    for go in plan:
        go()

    for m in range(micros):
        for d in range(n_e):
            if d:
                d_copy(m, d).wait_send()
                z_copy(m, d).wait_send()
            for da in range(n_a):
                if da:
                    f_copy(m, d, da).wait_send()
                    y_copy(m, d, da).wait_send()
                if pair > 1:
                    c_copy(m, d, da).wait_send()
        if pair > 1:
            for h in range(len(halves)):
                for da in range(n_a):
                    p_copy(m, h, da).wait_send()

        @pl.when(p < n_p - 1)
        def _():
            relay(m).wait_send()


def local(mesh_shape, tokens, gains, route_ids, route_weights, picks, w_gate, w_up, w_down):
    n_p, n_t, n_e = mesh_shape
    micros, toks, model_width = tokens.shape
    route_count = route_ids.shape[3]
    quarter = toks // n_t
    capacity = 4 * quarter * route_count // (3 * n_e)
    width = model_width // n_t
    pair = 2 if n_t % 2 == 0 else 1
    n_a = n_t // pair
    rows_ge = -(-n_t * capacity // 8) * 8
    cut = (n_e + 1) // 2
    rows = cut * rows_ge
    hidden_width = w_gate.shape[3]

    ids = route_ids[0].transpose(0, 2, 1)
    weights = route_weights[0].transpose(0, 2, 1)
    order = picks[0]

    sizes = (micros, n_p, n_t, n_e, pair, rows_ge, width, capacity)
    dma = pltpu.SemaphoreType.DMA
    vmem = pl.BlockSpec(memory_space=pltpu.VMEM)
    pinned = pl.BlockSpec(memory_space=pl.ANY)
    return pl.pallas_call(
        functools.partial(layer_kernel, sizes),
        out_shape=jax.ShapeDtypeStruct((1, micros, toks, width), BF16),
        in_specs=[pinned] * 8,
        out_specs=vmem,
        scratch_shapes=[
            pltpu.VMEM(gains.shape, F32),
            pltpu.VMEM(ids.shape, jnp.int32),
            pltpu.VMEM(weights.shape, F32),
            pltpu.VMEM(order.shape, jnp.int32),
            pltpu.VMEM((micros, n_e, rows_ge, toks), BF16),
            pltpu.VMEM((micros, n_e, 2 * toks, rows_ge), BF16),
            pltpu.VMEM((micros, toks, width), BF16),
            pltpu.VMEM((micros, toks, width), BF16),
            pltpu.VMEM((micros, n_e, rows_ge, width), BF16),
            pltpu.VMEM((micros, n_t, n_e, rows_ge, width), BF16),
            pltpu.VMEM(w_gate.shape[2:], BF16),
            pltpu.VMEM(w_up.shape[2:], BF16),
            pltpu.VMEM(w_down.shape[2:], BF16),
            pltpu.VMEM((rows, hidden_width), F32),
            pltpu.VMEM((rows, hidden_width), F32),
            pltpu.VMEM((micros, 2, n_a, rows, width), BF16),
            pltpu.VMEM((micros, 2, n_a, rows, width), BF16),
            pltpu.VMEM((micros, 2, n_a, rows, width), BF16),
            pltpu.VMEM((micros, n_e, n_a, rows_ge, width), BF16),
            pltpu.VMEM((micros, n_e, n_a, rows_ge, width), BF16),
            pltpu.VMEM((micros, n_e, rows_ge, width), BF16),
            pltpu.VMEM((micros, n_e, rows_ge, width), BF16),
            dma((4,)), dma((3,)), dma((micros,)), dma((micros,)), dma((micros,)),
            dma((micros, n_e)), dma((micros, n_e)),
            dma((micros, n_e, n_a)), dma((micros, n_e, n_a)),
            dma((micros, n_e, n_a)), dma((micros, n_e, n_a)),
            dma((micros, 2, n_a)), dma((micros, 2, n_a)),
            dma((micros, n_e, n_a)), dma((micros, n_e, n_a)),
            dma((micros, n_e)), dma((micros, n_e)),
        ],
        compiler_params=pltpu.CompilerParams(
            collective_id=0, has_side_effects=True, vmem_limit_bytes=67043328
        ),
    )(tokens, gains, ids, weights, order, w_gate, w_up, w_down)


def solution(mesh):
    mesh_shape = (mesh.shape["pipe"], mesh.shape["tensor"], mesh.shape["expert"])
    return jax.shard_map(
        functools.partial(local, mesh_shape),
        mesh=mesh,
        in_specs=(
            P(None, "expert", None),
            P("pipe", None),
            P("pipe", None, "expert", None),
            P("pipe", None, "expert", None),
            P("pipe", None, "expert", None),
            P("pipe", "expert", None, "tensor"),
            P("pipe", "expert", None, "tensor"),
            P("pipe", "expert", "tensor", None),
        ),
        out_specs=P("pipe", None, "expert", "tensor"),
        check_vma=False,
    )
```
